32 devices in a mesh: part: 1 (over z), data: 4 (over y), model: 8 (over x, core).
Axes of the slice: x: 4, y: 4, z: 1, core: 2. Of those that a mesh axis runs over, the one named last changes fastest.
The devices are a block of a 4x4x8 slice.
Arguments:
- x: bfloat16 [2, 16, 1024, 2048], P(None, ('part', 'data'), 'model')
- lengths: int32 [2, 16], P(None, ('part', 'data'))
- norm_gain: bfloat16 [2, 2048], P(None, 'data')
- w_in: bfloat16 [2, 2048, 18432], P(None, 'data', 'model')
- w_kv: bfloat16 [2, 2048, 256], P(None, 'data')
- w_out: bfloat16 [2, 10240, 2048], P(None, 'model', 'data')
Outputs:
- output: bfloat16 [2, 16, 1024, 2048], P(None, ('part', 'data'), 'model')
All inputs are finite; a program needn't handle non-finite values.
Results may differ from the reference program's by a relative error of at most 0.014422.
Values are sent between devices in bfloat16 or wider.
A program may use at most 768 MiB of HBM per device.

```python
import math
import jax
import jax.numpy as jnp
from jax import lax

N_MICRO = 2
N_LAYERS = 2
N_SEQS = 16
SEQ_LEN = 1024
D_MODEL = 2048
N_HEADS = 16
HEAD_DIM = 128
D_FF = 8192
MODEL_SHARDS = 8
FF_HEAD = D_FF // N_HEADS
UNIT_IN = HEAD_DIM + 2 * FF_HEAD
UNIT_OUT = HEAD_DIM + FF_HEAD
SHARD_ROWS = (N_HEADS // MODEL_SHARDS) * UNIT_OUT
NORM_EPS = 1e-6
NEG_BIG = -1e30
Q_GAIN = math.sqrt(max(math.log(SEQ_LEN / 8.0), 1.0))


def setup_inputs(seed: int = 0, part: int = 0) -> dict:
    part_keys = jax.random.split(jax.random.fold_in(jax.random.key(seed), part), 2)
    shared_keys = jax.random.split(jax.random.key(seed + 1), 4)
    x_act = jax.random.normal(part_keys[0], (N_MICRO, N_SEQS, SEQ_LEN, D_MODEL), jnp.float32)
    seq_lens = jax.random.randint(part_keys[1], (N_MICRO, N_SEQS), SEQ_LEN // 4, SEQ_LEN + 1)
    seq_lens = seq_lens.at[0, 0].set(SEQ_LEN).at[1, 0].set(SEQ_LEN // 4)
    gain_vals = jax.random.uniform(shared_keys[0], (N_LAYERS, D_MODEL), jnp.float32, 0.5, 1.5)
    col_scale = jnp.concatenate([jnp.full((HEAD_DIM,), Q_GAIN, jnp.float32), jnp.ones((2 * FF_HEAD,), jnp.float32)]) * (D_MODEL ** -0.5)
    w_in_vals = jax.random.normal(shared_keys[1], (N_LAYERS, D_MODEL, N_HEADS, UNIT_IN), jnp.float32) * col_scale
    w_kv_vals = jax.random.normal(shared_keys[2], (N_LAYERS, D_MODEL, 2 * HEAD_DIM), jnp.float32) * (D_MODEL ** -0.5)
    row_scale = jnp.concatenate([jnp.full((HEAD_DIM,), (N_HEADS * HEAD_DIM) ** -0.5, jnp.float32), jnp.full((FF_HEAD,), D_FF ** -0.5, jnp.float32)])
    w_out_vals = jax.random.normal(shared_keys[3], (N_LAYERS, N_HEADS, UNIT_OUT, D_MODEL), jnp.float32) * row_scale[:, None]
    return {
        "x": x_act.astype(jnp.bfloat16),
        "lengths": seq_lens.astype(jnp.int32),
        "norm_gain": gain_vals.astype(jnp.bfloat16),
        "w_in": w_in_vals.reshape(N_LAYERS, D_MODEL, N_HEADS * UNIT_IN).astype(jnp.bfloat16),
        "w_kv": w_kv_vals.astype(jnp.bfloat16),
        "w_out": w_out_vals.reshape(N_LAYERS, N_HEADS * UNIT_OUT, D_MODEL).astype(jnp.bfloat16),
    }


def layer_one_seq(x_seq, seq_len, gain_vec, w_in_l, w_kv_l, w_out_l):
    x_f32 = x_seq.astype(jnp.float32)
    centered = x_f32 - jnp.mean(x_f32, axis=-1, keepdims=True)
    variance = jnp.mean(centered * centered, axis=-1, keepdims=True)
    h_act = (centered * lax.rsqrt(variance + NORM_EPS) * gain_vec.astype(jnp.float32)).astype(jnp.bfloat16)
    projected = jnp.dot(h_act, w_in_l, preferred_element_type=jnp.float32).astype(jnp.bfloat16)
    projected = projected.reshape(SEQ_LEN, N_HEADS, UNIT_IN)
    q_heads = projected[:, :, :HEAD_DIM]
    gate_act = projected[:, :, HEAD_DIM:HEAD_DIM + FF_HEAD]
    up_act = projected[:, :, HEAD_DIM + FF_HEAD:]
    kv_act = jnp.dot(h_act, w_kv_l, preferred_element_type=jnp.float32).astype(jnp.bfloat16)
    k_act = kv_act[:, :HEAD_DIM]
    v_act = kv_act[:, HEAD_DIM:]
    scores = jnp.einsum("qhc,kc->hqk", q_heads.astype(jnp.float32), k_act.astype(jnp.float32)) * (1.0 / math.sqrt(HEAD_DIM))
    positions = jnp.arange(SEQ_LEN)
    allowed = (positions[None, :] <= positions[:, None]) & (positions[None, :] < seq_len)
    scores = jnp.where(allowed[None], scores, NEG_BIG)
    attn_probs = jax.nn.softmax(scores, axis=-1).astype(jnp.bfloat16)
    attn_out = jnp.einsum("hqk,kc->qhc", attn_probs.astype(jnp.float32), v_act.astype(jnp.float32)).astype(jnp.bfloat16)
    mlp_out = (jax.nn.silu(gate_act.astype(jnp.float32)) * up_act.astype(jnp.float32)).astype(jnp.bfloat16)
    joined = jnp.concatenate([attn_out, mlp_out], axis=-1).reshape(SEQ_LEN, MODEL_SHARDS, SHARD_ROWS)
    w_groups = w_out_l.reshape(MODEL_SHARDS, SHARD_ROWS, D_MODEL)

    def add_group(running, group_pair):
        rows_in, w_rows = group_pair
        group_sum = jnp.dot(rows_in, w_rows, preferred_element_type=jnp.float32).astype(jnp.bfloat16)
        return running + group_sum.astype(jnp.float32), None

    z_sum, _ = lax.scan(add_group, jnp.zeros((SEQ_LEN, D_MODEL), jnp.float32), (jnp.swapaxes(joined, 0, 1), w_groups))
    return (x_f32 + z_sum).astype(jnp.bfloat16)


def reference(x, lengths, norm_gain, w_in, w_kv, w_out):
    seqs_x = x.reshape(N_MICRO * N_SEQS, SEQ_LEN, D_MODEL)
    seqs_len = lengths.reshape(N_MICRO * N_SEQS)

    def run_seq(seq_item):
        x_seq, seq_len = seq_item

        def one_layer(carry_x, weights):
            gain_l, w_in_l, w_kv_l, w_out_l = weights
            return layer_one_seq(carry_x, seq_len, gain_l, w_in_l, w_kv_l, w_out_l), None

        final_x, _ = lax.scan(one_layer, x_seq, (norm_gain, w_in, w_kv, w_out))
        return final_x

    y_all = lax.map(run_seq, (seqs_x, seqs_len))
    return y_all.reshape(N_MICRO, N_SEQS, SEQ_LEN, D_MODEL)
```

```python
import math
import jax
import jax.numpy as jnp
from jax import lax
from jax.sharding import PartitionSpec as P

NORM_EPS = 1e-6
NEG_BIG = -1e30


def layer_norm(x_act, gain_vec):
    x_f32 = x_act.astype(jnp.float32)
    centered = x_f32 - jnp.mean(x_f32, axis=-1, keepdims=True)
    variance = jnp.mean(centered * centered, axis=-1, keepdims=True)
    return (centered * lax.rsqrt(variance + NORM_EPS) * gain_vec.astype(jnp.float32)).astype(jnp.bfloat16)


def attention(q_heads, k_all, v_all, seq_lens, q_offset):
    q_len = q_heads.shape[2]
    k_len = k_all.shape[1]
    head_dim = k_all.shape[2]
    scores = jnp.einsum("gbqc,bkc->bgqk", q_heads, k_all, preferred_element_type=jnp.float32) * (1.0 / math.sqrt(head_dim))
    q_pos = q_offset + lax.broadcasted_iota(jnp.int32, (q_len, 1), 0)
    k_pos = lax.broadcasted_iota(jnp.int32, (1, k_len), 1)
    allowed = (k_pos <= q_pos)[None, None] & (k_pos[None, None] < seq_lens[:, None, None, None])
    scores = jnp.where(allowed, scores, NEG_BIG)
    probs = jax.nn.softmax(scores, axis=-1).astype(jnp.bfloat16)
    return jnp.einsum("bgqk,bkc->gbqc", probs, v_all, preferred_element_type=jnp.float32).astype(jnp.bfloat16)


def solution(mesh):
    n_model = mesh.shape["model"]
    n_data = mesh.shape["data"]
    act_spec = P(None, ("part", "data"), "model", None)
    ring = ("model", "data")
    out_splits = (1, 2)

    def gather(arr, axes, axis):
        return lax.all_gather(arr, axes, axis=axis, tiled=True)

    def layers_fn(x_blk, len_blk, gain_blk, w_in_blk, w_kv_blk, w_out_blk):
        n_layers, feat, in_loc = w_in_blk.shape
        head_dim = w_kv_blk.shape[2] // 2
        out_loc = w_out_blk.shape[1]
        heads_loc = (out_loc - (in_loc - out_loc)) // head_dim
        unit_in = in_loc // heads_loc
        unit_out = out_loc // heads_loc
        ff_head = unit_out - head_dim
        n_micro, n_seqs, t_loc, d_model = x_blk.shape
        n_batch = n_micro * n_seqs
        rows = n_batch * t_loc
        lens = len_blk.reshape(n_batch)
        q_offset = lax.axis_index("model") * t_loc

        small = jnp.concatenate([w_kv_blk, jnp.broadcast_to(gain_blk[..., None], gain_blk.shape + (head_dim,))], axis=2)
        small = gather(small, "data", 1)
        hidden = x_blk.reshape(rows, d_model)
        for layer in range(n_layers):
            w_ins = []
            for c in range(heads_loc):
                piece = w_in_blk[layer, :, c * unit_in:(c + 1) * unit_in]
                piece = gather(piece, ring, 0)
                w_ins.append(piece.reshape(n_model, d_model, unit_in))
            splits = out_splits[layer]
            col = feat // splits
            w_outs = []
            for c in range(splits):
                piece = w_out_blk[layer, :, c * col:(c + 1) * col]
                piece = gather(piece, ring, 0)
                w_outs.append(piece.reshape(n_model, n_data, out_loc, col))

            h = layer_norm(hidden, small[layer, :, 2 * head_dim])
            kv = jnp.dot(h, small[layer, :, :2 * head_dim], preferred_element_type=jnp.float32).astype(jnp.bfloat16)
            kv = gather(kv.reshape(n_batch, t_loc, 2 * head_dim), "model", 1)
            joined = []
            for c in range(heads_loc):
                proj = jnp.einsum("td,gdf->gtf", h, w_ins[c], preferred_element_type=jnp.float32).astype(jnp.bfloat16)
                gate = proj[..., head_dim:head_dim + ff_head].astype(jnp.float32)
                up = proj[..., head_dim + ff_head:].astype(jnp.float32)
                m = (jax.nn.silu(gate) * up).astype(jnp.bfloat16)
                q = proj[..., :head_dim].reshape(n_model, n_batch, t_loc, head_dim)
                o = attention(q, kv[..., :head_dim], kv[..., head_dim:], lens, q_offset)
                joined += [o.reshape(n_model, rows, head_dim), m]
            joined = jnp.concatenate(joined, axis=-1)
            zs = []
            for c in range(splits):
                z = jnp.zeros((n_data, rows, col), jnp.float32)
                for g in range(n_model):
                    zg = jnp.einsum("tr,yrc->ytc", joined[g], w_outs[c][g], preferred_element_type=jnp.float32)
                    z = z + zg.astype(jnp.bfloat16).astype(jnp.float32)
                zs.append(z)
            z = jnp.concatenate(zs, axis=-1).transpose(1, 0, 2).reshape(rows, d_model)
            hidden = (hidden.astype(jnp.float32) + z).astype(jnp.bfloat16)
        return hidden.reshape(x_blk.shape)

    return jax.shard_map(
        layers_fn,
        mesh=mesh,
        in_specs=(act_spec, P(None, ("part", "data")), P(None, "data"), P(None, "data", "model"), P(None, "data", None), P(None, "model", "data")),
        out_specs=act_spec,
        check_vma=False,
    )
```

```python
import functools
import math
import jax
import jax.numpy as jnp
from jax import lax
from jax.experimental import pallas as pl
from jax.experimental.pallas import tpu as pltpu
from jax.sharding import PartitionSpec as P

NORM_EPS = 1e-6
NEG_BIG = -1e30
VMEM_LIMIT = 60 * 1024 * 1024
FF_TILE = 256


def layer_norm(x_act, gain_vec):
    x_f32 = x_act.astype(jnp.float32)
    centered = x_f32 - jnp.mean(x_f32, axis=-1, keepdims=True)
    variance = jnp.mean(centered * centered, axis=-1, keepdims=True)
    return (centered * lax.rsqrt(variance + NORM_EPS) * gain_vec.astype(jnp.float32)).astype(jnp.bfloat16)


def heads_kernel(n_heads, head_dim, ff_head, meta_ref, h_ref, kv_ref, w_ref, o_ref, q_ref):
    unit_in = head_dim + 2 * ff_head
    unit_out = head_dim + ff_head
    n_blocks, n_batch, t_loc, _ = kv_ref.shape
    k_len = n_blocks * t_loc
    tiles = ff_head // FF_TILE

    w_q = jnp.concatenate([w_ref[0, :, i * unit_in:i * unit_in + head_dim] for i in range(n_heads)], axis=1)
    q_ref[...] = jnp.dot(h_ref[...], w_q, preferred_element_type=jnp.float32).astype(jnp.bfloat16)

    @pl.loop(0, n_heads * tiles)
    def _(step):
        head = step // tiles
        tile = step % tiles
        g_at = pl.multiple_of(head * unit_in + head_dim + tile * FF_TILE, 128)
        u_at = pl.multiple_of(head * unit_in + head_dim + ff_head + tile * FF_TILE, 128)
        m_at = pl.multiple_of(head * unit_out + head_dim + tile * FF_TILE, 128)
        gate = jnp.dot(h_ref[...], w_ref[0, :, pl.ds(g_at, FF_TILE)], preferred_element_type=jnp.float32)
        up = jnp.dot(h_ref[...], w_ref[0, :, pl.ds(u_at, FF_TILE)], preferred_element_type=jnp.float32)
        gate = gate.astype(jnp.bfloat16).astype(jnp.float32)
        up = up.astype(jnp.bfloat16).astype(jnp.float32)
        o_ref[0, :, pl.ds(m_at, FF_TILE)] = (gate * jax.nn.sigmoid(gate) * up).astype(jnp.bfloat16)

    @pl.loop(0, n_batch)
    def _(b):
        at = pl.multiple_of(b * t_loc, t_loc)
        q = jnp.concatenate([q_ref[pl.ds(at, t_loc), i * head_dim:(i + 1) * head_dim] for i in range(n_heads)], axis=0)
        k = kv_ref[:, b, :, :head_dim].reshape(k_len, head_dim)
        v = kv_ref[:, b, :, head_dim:].reshape(k_len, head_dim)
        s = lax.dot_general(q, k, (((1,), (1,)), ((), ())), preferred_element_type=jnp.float32) * (1.0 / math.sqrt(head_dim))
        q_pos = meta_ref[n_batch] + lax.broadcasted_iota(jnp.int32, (t_loc, k_len), 0)
        k_pos = lax.broadcasted_iota(jnp.int32, (t_loc, k_len), 1)
        allowed = k_pos <= jnp.minimum(q_pos, meta_ref[b] - 1)
        s = jnp.where(jnp.concatenate([allowed] * n_heads, axis=0), s, NEG_BIG)
        e = jnp.exp(s - jnp.max(s, axis=-1, keepdims=True))
        p = (e * (1.0 / jnp.sum(e, axis=-1, keepdims=True))).astype(jnp.bfloat16)
        o = jnp.dot(p, v, preferred_element_type=jnp.float32).astype(jnp.bfloat16)
        for i in range(n_heads):
            o_ref[0, pl.ds(at, t_loc), i * unit_out:i * unit_out + head_dim] = o[i * t_loc:(i + 1) * t_loc]


def out_kernel(x_ref, a_ref, w_ref, y_ref, acc_ref):
    group = pl.program_id(1)
    col = w_ref.shape[3]

    @pl.when(group == 0)
    def _():
        acc_ref[...] = jnp.zeros_like(acc_ref)

    for c in range(w_ref.shape[1]):
        z = jnp.dot(a_ref[0], w_ref[0, c], preferred_element_type=jnp.float32)
        acc_ref[:, c * col:(c + 1) * col] += z.astype(jnp.bfloat16).astype(jnp.float32)

    @pl.when(group == pl.num_programs(1) - 1)
    def _():
        y_ref[...] = (x_ref[...].astype(jnp.float32) + acc_ref[...]).astype(jnp.bfloat16)


def project_heads(meta, h, kv, w_in, n_heads, head_dim, ff_head):
    n_groups, d_model, in_loc = w_in.shape
    rows = h.shape[0]
    out_loc = n_heads * (head_dim + ff_head)
    whole = pl.Buffered(1)
    return pl.pallas_call(
        functools.partial(heads_kernel, n_heads, head_dim, ff_head),
        grid=(n_groups,),
        in_specs=[
            pl.BlockSpec(memory_space=pltpu.SMEM),
            pl.BlockSpec(h.shape, lambda g: (0, 0), pipeline_mode=whole),
            pl.BlockSpec(kv.shape, lambda g: (0, 0, 0, 0), pipeline_mode=whole),
            pl.BlockSpec((1, d_model, in_loc), lambda g: (g, 0, 0)),
        ],
        out_specs=pl.BlockSpec((1, rows, out_loc), lambda g: (g, 0, 0)),
        out_shape=jax.ShapeDtypeStruct((n_groups, rows, out_loc), jnp.bfloat16),
        scratch_shapes=[pltpu.VMEM((rows, n_heads * head_dim), jnp.bfloat16)],
        compiler_params=pltpu.CompilerParams(vmem_limit_bytes=VMEM_LIMIT, dimension_semantics=("arbitrary",)),
        cost_estimate=pl.CostEstimate(flops=2 * rows * d_model * in_loc * n_groups, bytes_accessed=2 * w_in.size, transcendentals=0),
        name="project_heads",
    )(meta, h, kv, w_in)


def project_out(x, joined, w_out):
    n_groups, n_data, out_loc, col = w_out.shape
    rows, d_model = x.shape
    per = 2 if n_data % 2 == 0 else 1
    return pl.pallas_call(
        out_kernel,
        grid=(n_data // per, n_groups),
        in_specs=[
            pl.BlockSpec((rows, per * col), lambda c, g: (0, c)),
            pl.BlockSpec((1, rows, out_loc), lambda c, g: (g, 0, 0)),
            pl.BlockSpec((1, per, out_loc, col), lambda c, g: (g, c, 0, 0)),
        ],
        out_specs=pl.BlockSpec((rows, per * col), lambda c, g: (0, c)),
        out_shape=jax.ShapeDtypeStruct((rows, d_model), jnp.bfloat16),
        scratch_shapes=[pltpu.VMEM((rows, per * col), jnp.float32)],
        compiler_params=pltpu.CompilerParams(vmem_limit_bytes=VMEM_LIMIT, dimension_semantics=("arbitrary", "arbitrary")),
        cost_estimate=pl.CostEstimate(flops=2 * rows * d_model * out_loc * n_groups, bytes_accessed=2 * w_out.size, transcendentals=0),
        name="project_out",
    )(x, joined, w_out)


def stack_by_shift(arr, axis, size, stride):
    n = size // stride
    parts = [arr]
    for r in range(1, n):
        parts.append(lax.ppermute(arr, axis, [(i, (i + r * stride) % size) for i in range(size)]))
    return jnp.stack(parts)


def absolute_order(rel, mine, n):
    return jnp.concatenate([lax.dynamic_slice_in_dim(rel, lax.rem(mine - i + n, n), 1, 0) for i in range(n)])


def gather_model(arr, n_model):
    me = lax.axis_index("model")
    half = n_model // 2
    mine = stack_by_shift(arr, "model", n_model, 2)
    other = lax.ppermute(mine, "model", [(i, i ^ 1) for i in range(n_model)])
    first = lax.rem(me, 2) == 0
    both = jnp.stack([jnp.where(first, mine, other), jnp.where(first, other, mine)], axis=1)
    both = absolute_order(both, me // 2, half)
    return both.reshape((n_model,) + arr.shape)


def solution(mesh):
    n_model = mesh.shape["model"]
    n_data = mesh.shape["data"]
    act_spec = P(None, ("part", "data"), "model", None)
    ring = ("model", "data")

    def gather(arr):
        return lax.all_gather(arr, ring, axis=0, tiled=True)

    def layers_fn(x_blk, len_blk, gain_blk, w_in_blk, w_kv_blk, w_out_blk):
        n_layers, feat, in_loc = w_in_blk.shape
        head_dim = w_kv_blk.shape[2] // 2
        out_loc = w_out_blk.shape[1]
        heads_loc = (out_loc - (in_loc - out_loc)) // head_dim
        ff_head = out_loc // heads_loc - head_dim
        n_micro, n_seqs, t_loc, d_model = x_blk.shape
        n_batch = n_micro * n_seqs
        rows = n_batch * t_loc
        me_data = lax.axis_index("data")
        q_offset = lax.axis_index("model") * t_loc
        meta = jnp.concatenate([len_blk.reshape(n_batch), q_offset[None]]).astype(jnp.int32)

        weights = []
        for layer in range(n_layers):
            w_in = gather(w_in_blk[layer]).reshape(n_model, d_model, in_loc)
            w_out = gather(w_out_blk[layer]).reshape(n_model, n_data, out_loc, feat)
            weights.append((w_in, w_out))

        small = jnp.concatenate([w_kv_blk, jnp.broadcast_to(gain_blk[..., None], gain_blk.shape + (head_dim,))], axis=2)
        small = absolute_order(stack_by_shift(small, "data", n_data, 1), me_data, n_data)
        small = small.transpose(1, 0, 2, 3).reshape(n_layers, d_model, 3 * head_dim)

        hidden = x_blk.reshape(rows, d_model)
        for layer, (w_in, w_out) in enumerate(weights):
            h = layer_norm(hidden, small[layer, :, 2 * head_dim])
            kv = jnp.dot(h, small[layer, :, :2 * head_dim], preferred_element_type=jnp.float32).astype(jnp.bfloat16)
            kv = gather_model(kv.reshape(n_batch, t_loc, 2 * head_dim), n_model)
            joined = project_heads(meta, h, kv, w_in, heads_loc, head_dim, ff_head)
            hidden = project_out(hidden, joined, w_out)
        return hidden.reshape(x_blk.shape)

    return jax.shard_map(
        layers_fn,
        mesh=mesh,
        in_specs=(act_spec, P(None, ("part", "data")), P(None, "data"), P(None, "data", "model"), P(None, "data", None), P(None, "model", "data")),
        out_specs=act_spec,
        check_vma=False,
    )
```

```python
import functools
import math
import jax
import jax.numpy as jnp
from jax import lax
from jax.experimental import pallas as pl
from jax.experimental.pallas import tpu as pltpu
from jax.sharding import PartitionSpec as P

NORM_EPS = 1e-6
NEG_BIG = -1e30
VMEM_LIMIT = 60 * 1024 * 1024
FF_TILE = 256


def layer_norm(x_act, gain_vec):
    x_f32 = x_act.astype(jnp.float32)
    centered = x_f32 - jnp.mean(x_f32, axis=-1, keepdims=True)
    variance = jnp.mean(centered * centered, axis=-1, keepdims=True)
    return (centered * lax.rsqrt(variance + NORM_EPS) * gain_vec.astype(jnp.float32)).astype(jnp.bfloat16)


def attend_all(n_heads, head_dim, meta_ref, q_ref, kv_ref, o_ref, unit_out):
    n_blocks, n_batch, t_loc, _ = kv_ref.shape
    k_len = n_blocks * t_loc
    exponent = math.log2(math.e) / math.sqrt(head_dim)

    @pl.loop(0, n_batch)
    def _(b):
        at = pl.multiple_of(b * t_loc, t_loc)
        q = jnp.concatenate([q_ref[pl.ds(at, t_loc), i * head_dim:(i + 1) * head_dim] for i in range(n_heads)], axis=0)
        k = kv_ref[:, b, :, :head_dim].reshape(k_len, head_dim)
        v = kv_ref[:, b, :, head_dim:].reshape(k_len, head_dim)
        s = lax.dot_general(q, k, (((1,), (1,)), ((), ())), preferred_element_type=jnp.float32)
        q_pos = meta_ref[n_batch] + lax.broadcasted_iota(jnp.int32, (t_loc, 1), 0)
        k_pos = lax.broadcasted_iota(jnp.int32, (t_loc, k_len), 1)
        allowed = k_pos <= jnp.minimum(q_pos, meta_ref[b] - 1)
        s = jnp.where(jnp.concatenate([allowed] * n_heads, axis=0), s, NEG_BIG)
        e = jnp.exp2((s - jnp.max(s, axis=-1, keepdims=True)) * exponent)
        p = (e * (1.0 / jnp.sum(e, axis=-1, keepdims=True))).astype(jnp.bfloat16)
        o = jnp.dot(p, v, preferred_element_type=jnp.float32).astype(jnp.bfloat16)
        for i in range(n_heads):
            o_ref[0, pl.ds(at, t_loc), i * unit_out:i * unit_out + head_dim] = o[i * t_loc:(i + 1) * t_loc]


def gate_all(n_heads, head_dim, ff_head, skip, h_ref, w_ref, o_ref):
    unit_in = skip + 2 * ff_head
    unit_out = head_dim + ff_head
    tiles = ff_head // FF_TILE

    @pl.loop(0, n_heads * tiles)
    def _(step):
        head = step // tiles
        tile = step % tiles
        g_at = pl.multiple_of(head * unit_in + skip + tile * FF_TILE, 128)
        u_at = pl.multiple_of(head * unit_in + skip + ff_head + tile * FF_TILE, 128)
        m_at = pl.multiple_of(head * unit_out + head_dim + tile * FF_TILE, 128)
        gate = jnp.dot(h_ref[...], w_ref[0, :, pl.ds(g_at, FF_TILE)], preferred_element_type=jnp.float32)
        up = jnp.dot(h_ref[...], w_ref[0, :, pl.ds(u_at, FF_TILE)], preferred_element_type=jnp.float32)
        gate = gate.astype(jnp.bfloat16).astype(jnp.float32)
        up = up.astype(jnp.bfloat16).astype(jnp.float32)
        o_ref[0, :, pl.ds(m_at, FF_TILE)] = (gate * jax.nn.sigmoid(gate) * up).astype(jnp.bfloat16)


def heads_kernel(n_heads, head_dim, ff_head, meta_ref, h_ref, kv_ref, w_ref, o_ref, q_ref):
    unit_in = head_dim + 2 * ff_head
    w_q = jnp.concatenate([w_ref[0, :, i * unit_in:i * unit_in + head_dim] for i in range(n_heads)], axis=1)
    q_ref[...] = jnp.dot(h_ref[...], w_q, preferred_element_type=jnp.float32).astype(jnp.bfloat16)
    gate_all(n_heads, head_dim, ff_head, head_dim, h_ref, w_ref, o_ref)
    attend_all(n_heads, head_dim, meta_ref, q_ref, kv_ref, o_ref, head_dim + ff_head)


def attend_kernel(n_heads, head_dim, meta_ref, h_ref, kv_ref, w_ref, o_ref, q_ref):
    _, n_data, _, feat = w_ref.shape
    width = n_heads * head_dim
    w_q = jnp.concatenate([w_ref[0, y, :, i:i + width] for y in range(n_data) for i in range(0, feat, width)], axis=0)
    q_ref[...] = jnp.dot(h_ref[...], w_q, preferred_element_type=jnp.float32).astype(jnp.bfloat16)
    attend_all(n_heads, head_dim, meta_ref, q_ref, kv_ref, o_ref, head_dim)


def gate_kernel(n_heads, head_dim, ff_head, h_ref, a_ref, w_ref, o_ref):
    unit_out = head_dim + ff_head
    for i in range(n_heads):
        o_ref[0, :, i * unit_out:i * unit_out + head_dim] = a_ref[0, :, i * head_dim:(i + 1) * head_dim]
    gate_all(n_heads, head_dim, ff_head, 0, h_ref, w_ref, o_ref)


def out_kernel(at, x_ref, a_ref, w_ref, y_ref, acc_ref):
    group = pl.program_id(1)
    _, per, _, width = w_ref.shape
    feat = x_ref.shape[1] // per

    @pl.when(group == 0)
    def _():
        acc_ref[...] = jnp.zeros_like(acc_ref)

    w = jnp.concatenate([w_ref[0, c] for c in range(per)], axis=1)
    z = jnp.dot(a_ref[0], w, preferred_element_type=jnp.float32)
    acc_ref[...] += z.astype(jnp.bfloat16).astype(jnp.float32)

    @pl.when(group == pl.num_programs(1) - 1)
    def _():
        if width < feat:
            y_ref[...] = x_ref[...]
        for c in range(per):
            here = slice(c * feat + at, c * feat + at + width)
            y_ref[:, here] = (x_ref[:, here].astype(jnp.float32) + acc_ref[:, c * width:(c + 1) * width]).astype(jnp.bfloat16)


def group_call(kernel, args, specs, rows, out_cols, n_groups, flops, scratch=()):
    return pl.pallas_call(
        kernel,
        grid=(n_groups,),
        in_specs=specs,
        out_specs=pl.BlockSpec((1, rows, out_cols), lambda g: (g, 0, 0)),
        out_shape=jax.ShapeDtypeStruct((n_groups, rows, out_cols), jnp.bfloat16),
        scratch_shapes=list(scratch),
        compiler_params=pltpu.CompilerParams(vmem_limit_bytes=VMEM_LIMIT, dimension_semantics=("arbitrary",)),
        cost_estimate=pl.CostEstimate(flops=flops, bytes_accessed=2 * args[-1].size, transcendentals=0),
    )(*args)


def whole(arr):
    zeros = (0,) * arr.ndim
    return pl.BlockSpec(arr.shape, lambda g: zeros, pipeline_mode=pl.Buffered(1))


def project_heads(meta, h, kv, w_in, n_heads, head_dim, ff_head):
    n_groups, d_model, in_loc = w_in.shape
    rows = h.shape[0]
    return group_call(
        functools.partial(heads_kernel, n_heads, head_dim, ff_head),
        (meta, h, kv, w_in),
        [pl.BlockSpec(memory_space=pltpu.SMEM), whole(h), whole(kv), pl.BlockSpec((1, d_model, in_loc), lambda g: (g, 0, 0))],
        rows, n_heads * (head_dim + ff_head), n_groups, 2 * rows * d_model * in_loc * n_groups,
        [pltpu.VMEM((rows, n_heads * head_dim), jnp.bfloat16)],
    )


def attend_heads(meta, h, kv, w_packed, n_heads, head_dim):
    n_groups, n_data, packed_rows, feat = w_packed.shape
    rows, d_model = h.shape
    width = n_heads * head_dim
    q_rows = feat * width // feat
    last = packed_rows // q_rows - 1
    return group_call(
        functools.partial(attend_kernel, n_heads, head_dim),
        (meta, h, kv, w_packed),
        [pl.BlockSpec(memory_space=pltpu.SMEM), whole(h), whole(kv), pl.BlockSpec((1, n_data, q_rows, feat), lambda g: (g, 0, last, 0))],
        rows, width, n_groups, 2 * rows * d_model * width * n_groups,
        [pltpu.VMEM((rows, width), jnp.bfloat16)],
    )


def gate_heads(h, attended, w_gu, n_heads, head_dim, ff_head):
    n_groups, d_model, cols = w_gu.shape
    rows = h.shape[0]
    return group_call(
        functools.partial(gate_kernel, n_heads, head_dim, ff_head),
        (h, attended, w_gu),
        [whole(h), pl.BlockSpec((1, rows, n_heads * head_dim), lambda g: (g, 0, 0)), pl.BlockSpec((1, d_model, cols), lambda g: (g, 0, 0))],
        rows, n_heads * (head_dim + ff_head), n_groups, 2 * rows * d_model * cols * n_groups,
    )


def pack_queries(w_q):
    feat, width = w_q.shape
    return jnp.concatenate([w_q[i:i + width] for i in range(0, feat, width)], axis=1)


def project_out(x, joined, w_out, at):
    n_groups, n_data, _, width = w_out.shape
    out_loc = joined.shape[2]
    rows, d_model = x.shape
    feat = d_model // n_data
    per = n_data if n_data * width <= 2 * feat else 2
    return pl.pallas_call(
        functools.partial(out_kernel, at),
        grid=(n_data // per, n_groups),
        in_specs=[
            pl.BlockSpec((rows, per * feat), lambda c, g: (0, c)),
            pl.BlockSpec((1, rows, out_loc), lambda c, g: (g, 0, 0)),
            pl.BlockSpec((1, per, out_loc, width), lambda c, g: (g, c, 0, 0)),
        ],
        out_specs=pl.BlockSpec((rows, per * feat), lambda c, g: (0, c)),
        out_shape=jax.ShapeDtypeStruct((rows, d_model), jnp.bfloat16),
        scratch_shapes=[pltpu.VMEM((rows, per * width), jnp.float32)],
        compiler_params=pltpu.CompilerParams(vmem_limit_bytes=VMEM_LIMIT, dimension_semantics=("arbitrary", "arbitrary")),
        cost_estimate=pl.CostEstimate(flops=2 * rows * n_data * width * out_loc * n_groups, bytes_accessed=2 * w_out.size, transcendentals=0),
        name="project_out",
    )(x, joined, w_out)


def stack_by_shift(arr, axis, size, stride):
    n = size // stride

    def shift(value, r):
        return lax.ppermute(value, axis, [(i, (i + r * stride) % size) for i in range(size)])

    if n != 4:
        return jnp.stack([arr] + [shift(arr, r) for r in range(1, n)])
    back, ahead = shift(arr, 1), shift(arr, -1)
    half = arr.shape[0] // 2
    across = jnp.concatenate([shift(back[:half], 1), shift(ahead[half:], -1)])
    return jnp.stack([arr, back, across, ahead])


def absolute_order(rel, mine, n):
    return jnp.concatenate([lax.dynamic_slice_in_dim(rel, lax.rem(mine - i + n, n), 1, 0) for i in range(n)])


def swap_pair(value, n_model):
    other = lax.ppermute(value, "model", [(i, i ^ 1) for i in range(n_model)])
    first = lax.rem(lax.axis_index("model"), 2) == 0
    return jnp.where(first, value, other), jnp.where(first, other, value)


def gather_model(arr, n_model):
    mine = stack_by_shift(arr, "model", n_model, 2)
    both = jnp.stack(swap_pair(mine, n_model), axis=1)
    both = absolute_order(both, lax.axis_index("model") // 2, n_model // 2)
    return both.reshape((n_model,) + arr.shape)


def gather_kv_weights(w_kv, n_data, n_model):
    n_layers, feat, cols = w_kv.shape
    first = lax.rem(lax.axis_index("model"), 2) == 0
    half = jnp.where(first, w_kv[..., :cols // 2], w_kv[..., cols // 2:])
    half = absolute_order(stack_by_shift(half, "data", n_data, 1), lax.axis_index("data"), n_data)
    whole = jnp.concatenate(swap_pair(half, n_model), axis=-1)
    return whole.transpose(1, 0, 2, 3).reshape(n_layers, n_data * feat, cols)


def solution(mesh):
    n_model = mesh.shape["model"]
    n_data = mesh.shape["data"]
    act_spec = P(None, ("part", "data"), "model", None)
    ring = ("model", "data")

    def gather(arr):
        return lax.all_gather(arr, ring, axis=0, tiled=True)

    def layers_fn(x_blk, len_blk, gain_blk, w_in_blk, w_kv_blk, w_out_blk):
        n_layers, feat, in_loc = w_in_blk.shape
        head_dim = w_kv_blk.shape[2] // 2
        out_loc = w_out_blk.shape[1]
        heads_loc = (out_loc - (in_loc - out_loc)) // head_dim
        ff_head = out_loc // heads_loc - head_dim
        n_micro, n_seqs, t_loc, d_model = x_blk.shape
        n_batch = n_micro * n_seqs
        rows = n_batch * t_loc
        q_offset = lax.axis_index("model") * t_loc
        meta = jnp.concatenate([len_blk.reshape(n_batch), q_offset[None]]).astype(jnp.int32)

        unit_in = in_loc // heads_loc
        weights = []
        for layer in range(n_layers):
            heads = [w_in_blk[layer, :, i * unit_in:(i + 1) * unit_in] for i in range(heads_loc)]
            piece = w_in_blk[layer] if layer == 0 else jnp.concatenate([w[:, head_dim:] for w in heads], axis=1)
            w_in = gather(piece).reshape(n_model, d_model, piece.shape[1])
            w_outs = []
            last = layer == n_layers - 1
            cuts = (0, feat * 3 // 4, feat) if last else (0, feat)
            for lo, hi in zip(cuts, cuts[1:]):
                piece = w_out_blk[layer, :, lo:hi]
                if not last:
                    after = [w_in_blk[layer + 1, :, j * unit_in:j * unit_in + head_dim] for j in range(heads_loc)]
                    piece = jnp.concatenate([piece, pack_queries(jnp.concatenate(after, axis=1))])
                w_out = gather(piece)
                w_outs.append((lo, w_out.reshape((n_model, n_data) + piece.shape)))
            weights.append((w_in, w_outs))

        gain = lax.all_gather(gain_blk, "data", axis=1, tiled=True)
        w_kv = gather_kv_weights(w_kv_blk, n_data, n_model)

        hidden = x_blk.reshape(rows, d_model)
        for layer, (w_in, w_outs) in enumerate(weights):
            h = layer_norm(hidden, gain[layer])
            kv = jnp.dot(h, w_kv[layer], preferred_element_type=jnp.float32).astype(jnp.bfloat16)
            kv = gather_model(kv.reshape(n_batch, t_loc, 2 * head_dim), n_model)
            if layer == 0:
                joined = project_heads(meta, h, kv, w_in, heads_loc, head_dim, ff_head)
            else:
                attended = attend_heads(meta, h, kv, weights[layer - 1][1][-1][1], heads_loc, head_dim)
                joined = gate_heads(h, attended, w_in, heads_loc, head_dim, ff_head)
            for at, w_out in w_outs:
                hidden = project_out(hidden, joined, w_out, at)
        return hidden.reshape(x_blk.shape)

    return jax.shard_map(
        layers_fn,
        mesh=mesh,
        in_specs=(act_spec, P(None, ("part", "data")), P(None, "data"), P(None, "data", "model"), P(None, "data", None), P(None, "model", "data")),
        out_specs=act_spec,
        check_vma=False,
    )
```

```python
import functools
import math
import jax
import jax.numpy as jnp
from jax import lax
from jax.experimental import pallas as pl
from jax.experimental.pallas import tpu as pltpu
from jax.sharding import PartitionSpec as P

NORM_EPS = 1e-6
NEG_BIG = -1e30
VMEM_LIMIT = 60 * 1024 * 1024
FF_TILE = 256


def layer_norm(x_act, gain_vec):
    x_f32 = x_act.astype(jnp.float32)
    centered = x_f32 - jnp.mean(x_f32, axis=-1, keepdims=True)
    variance = jnp.mean(centered * centered, axis=-1, keepdims=True)
    return (centered * lax.rsqrt(variance + NORM_EPS) * gain_vec.astype(jnp.float32)).astype(jnp.bfloat16)


def attend_all(n_heads, head_dim, meta_ref, q_ref, kv_ref, o_ref, unit_out):
    n_blocks, n_batch, t_loc, _ = kv_ref.shape
    k_len = n_blocks * t_loc
    exponent = math.log2(math.e) / math.sqrt(head_dim)

    @pl.loop(0, n_batch)
    def _(b):
        at = pl.multiple_of(b * t_loc, t_loc)
        q = jnp.concatenate([q_ref[pl.ds(at, t_loc), i * head_dim:(i + 1) * head_dim] for i in range(n_heads)], axis=0)
        k = kv_ref[:, b, :, :head_dim].reshape(k_len, head_dim)
        v = kv_ref[:, b, :, head_dim:].reshape(k_len, head_dim)
        s = lax.dot_general(q, k, (((1,), (1,)), ((), ())), preferred_element_type=jnp.float32)
        q_pos = meta_ref[n_batch] + lax.broadcasted_iota(jnp.int32, (t_loc, 1), 0)
        k_pos = lax.broadcasted_iota(jnp.int32, (t_loc, k_len), 1)
        allowed = k_pos <= jnp.minimum(q_pos, meta_ref[b] - 1)
        s = jnp.where(jnp.concatenate([allowed] * n_heads, axis=0), s, NEG_BIG)
        e = jnp.exp2((s - jnp.max(s, axis=-1, keepdims=True)) * exponent)
        p = (e * (1.0 / jnp.sum(e, axis=-1, keepdims=True))).astype(jnp.bfloat16)
        o = jnp.dot(p, v, preferred_element_type=jnp.float32).astype(jnp.bfloat16)
        for i in range(n_heads):
            o_ref[0, pl.ds(at, t_loc), i * unit_out:i * unit_out + head_dim] = o[i * t_loc:(i + 1) * t_loc]


def gate_all(n_heads, head_dim, ff_head, skip, h_ref, w_ref, o_ref):
    unit_in = skip + 2 * ff_head
    unit_out = head_dim + ff_head
    tiles = ff_head // FF_TILE

    @pl.loop(0, n_heads * tiles)
    def _(step):
        head = step // tiles
        tile = step % tiles
        g_at = pl.multiple_of(head * unit_in + skip + tile * FF_TILE, 128)
        u_at = pl.multiple_of(head * unit_in + skip + ff_head + tile * FF_TILE, 128)
        m_at = pl.multiple_of(head * unit_out + head_dim + tile * FF_TILE, 128)
        gate = jnp.dot(h_ref[...], w_ref[0, :, pl.ds(g_at, FF_TILE)], preferred_element_type=jnp.float32)
        up = jnp.dot(h_ref[...], w_ref[0, :, pl.ds(u_at, FF_TILE)], preferred_element_type=jnp.float32)
        gate = gate.astype(jnp.bfloat16).astype(jnp.float32)
        up = up.astype(jnp.bfloat16).astype(jnp.float32)
        o_ref[0, :, pl.ds(m_at, FF_TILE)] = (gate * jax.nn.sigmoid(gate) * up).astype(jnp.bfloat16)


def heads_kernel(n_heads, head_dim, ff_head, meta_ref, h_ref, kv_ref, w_ref, o_ref, q_ref):
    unit_in = head_dim + 2 * ff_head
    w_q = jnp.concatenate([w_ref[0, :, i * unit_in:i * unit_in + head_dim] for i in range(n_heads)], axis=1)
    q_ref[...] = jnp.dot(h_ref[...], w_q, preferred_element_type=jnp.float32).astype(jnp.bfloat16)
    gate_all(n_heads, head_dim, ff_head, head_dim, h_ref, w_ref, o_ref)
    attend_all(n_heads, head_dim, meta_ref, q_ref, kv_ref, o_ref, head_dim + ff_head)


def attend_kernel(n_heads, head_dim, meta_ref, h_ref, kv_ref, w_ref, o_ref, q_ref):
    _, n_data, _, feat = w_ref.shape
    width = n_heads * head_dim
    w_q = jnp.concatenate([w_ref[0, y, :, i:i + width] for y in range(n_data) for i in range(0, feat, width)], axis=0)
    q_ref[...] = jnp.dot(h_ref[...], w_q, preferred_element_type=jnp.float32).astype(jnp.bfloat16)
    attend_all(n_heads, head_dim, meta_ref, q_ref, kv_ref, o_ref, head_dim)


def gate_kernel(n_heads, head_dim, ff_head, h_ref, a_ref, w_ref, o_ref):
    unit_out = head_dim + ff_head
    for i in range(n_heads):
        o_ref[0, :, i * unit_out:i * unit_out + head_dim] = a_ref[0, :, i * head_dim:(i + 1) * head_dim]
    gate_all(n_heads, head_dim, ff_head, 0, h_ref, w_ref, o_ref)


def out_kernel(at, x_ref, a_ref, w_ref, y_ref, acc_ref):
    group = pl.program_id(1)
    _, per, _, width = w_ref.shape
    feat = x_ref.shape[1] // per

    @pl.when(group == 0)
    def _():
        acc_ref[...] = jnp.zeros_like(acc_ref)

    w = jnp.concatenate([w_ref[0, c] for c in range(per)], axis=1)
    z = jnp.dot(a_ref[0], w, preferred_element_type=jnp.float32)
    acc_ref[...] += z.astype(jnp.bfloat16).astype(jnp.float32)

    @pl.when(group == pl.num_programs(1) - 1)
    def _():
        if width < feat:
            y_ref[...] = x_ref[...]
        for c in range(per):
            here = slice(c * feat + at, c * feat + at + width)
            y_ref[:, here] = (x_ref[:, here].astype(jnp.float32) + acc_ref[:, c * width:(c + 1) * width]).astype(jnp.bfloat16)


def tail_kernel(at, x_ref, a_ref, w_ref, y_ref, part_ref, acc_ref, in_sem, out_sem):
    group = pl.program_id(0)
    _, per, _, width = w_ref.shape
    feat = x_ref.shape[1] // per

    def copy_in(c):
        return pltpu.make_async_copy(x_ref.at[:, pl.ds(c * feat + at, width)], part_ref.at[:, pl.ds(c * width, width)], in_sem.at[c])

    def copy_out(c):
        return pltpu.make_async_copy(part_ref.at[:, pl.ds(c * width, width)], y_ref.at[:, pl.ds(c * feat + at, width)], out_sem.at[c])

    @pl.when(group == 0)
    def _():
        for c in range(per):
            copy_in(c).start()
        acc_ref[...] = jnp.zeros_like(acc_ref)

    w = jnp.concatenate([w_ref[0, c] for c in range(per)], axis=1)
    z = jnp.dot(a_ref[0], w, preferred_element_type=jnp.float32)
    acc_ref[...] += z.astype(jnp.bfloat16).astype(jnp.float32)

    @pl.when(group == pl.num_programs(0) - 1)
    def _():
        for c in range(per):
            copy_in(c).wait()
        part_ref[...] = (part_ref[...].astype(jnp.float32) + acc_ref[...]).astype(jnp.bfloat16)
        for c in range(per):
            copy_out(c).start()
        for c in range(per):
            copy_out(c).wait()


def project_tail(x, joined, w_out, at):
    n_groups, n_data, out_loc, width = w_out.shape
    rows, d_model = x.shape
    return pl.pallas_call(
        functools.partial(tail_kernel, at),
        grid=(n_groups,),
        in_specs=[
            pl.BlockSpec(memory_space=pl.ANY),
            pl.BlockSpec((1, rows, out_loc), lambda g: (g, 0, 0)),
            pl.BlockSpec((1, n_data, out_loc, width), lambda g: (g, 0, 0, 0)),
        ],
        out_specs=pl.BlockSpec(memory_space=pl.ANY),
        out_shape=jax.ShapeDtypeStruct((rows, d_model), jnp.bfloat16),
        scratch_shapes=[
            pltpu.VMEM((rows, n_data * width), jnp.bfloat16),
            pltpu.VMEM((rows, n_data * width), jnp.float32),
            pltpu.SemaphoreType.DMA((n_data,)),
            pltpu.SemaphoreType.DMA((n_data,)),
        ],
        input_output_aliases={0: 0},
        compiler_params=pltpu.CompilerParams(vmem_limit_bytes=VMEM_LIMIT, dimension_semantics=("arbitrary",)),
        cost_estimate=pl.CostEstimate(flops=2 * rows * n_data * width * out_loc * n_groups, bytes_accessed=2 * w_out.size, transcendentals=0),
        name="project_tail",
    )(x, joined, w_out)


def group_call(kernel, args, specs, rows, out_cols, n_groups, flops, scratch=()):
    return pl.pallas_call(
        kernel,
        grid=(n_groups,),
        in_specs=specs,
        out_specs=pl.BlockSpec((1, rows, out_cols), lambda g: (g, 0, 0)),
        out_shape=jax.ShapeDtypeStruct((n_groups, rows, out_cols), jnp.bfloat16),
        scratch_shapes=list(scratch),
        compiler_params=pltpu.CompilerParams(vmem_limit_bytes=VMEM_LIMIT, dimension_semantics=("arbitrary",)),
        cost_estimate=pl.CostEstimate(flops=flops, bytes_accessed=2 * args[-1].size, transcendentals=0),
    )(*args)


def whole(arr):
    zeros = (0,) * arr.ndim
    return pl.BlockSpec(arr.shape, lambda g: zeros, pipeline_mode=pl.Buffered(1))


def project_heads(meta, h, kv, w_in, n_heads, head_dim, ff_head):
    n_groups, d_model, in_loc = w_in.shape
    rows = h.shape[0]
    return group_call(
        functools.partial(heads_kernel, n_heads, head_dim, ff_head),
        (meta, h, kv, w_in),
        [pl.BlockSpec(memory_space=pltpu.SMEM), whole(h), whole(kv), pl.BlockSpec((1, d_model, in_loc), lambda g: (g, 0, 0))],
        rows, n_heads * (head_dim + ff_head), n_groups, 2 * rows * d_model * in_loc * n_groups,
        [pltpu.VMEM((rows, n_heads * head_dim), jnp.bfloat16)],
    )


def attend_heads(meta, h, kv, w_packed, n_heads, head_dim):
    n_groups, n_data, packed_rows, feat = w_packed.shape
    rows, d_model = h.shape
    width = n_heads * head_dim
    q_rows = feat * width // feat
    last = packed_rows // q_rows - 1
    return group_call(
        functools.partial(attend_kernel, n_heads, head_dim),
        (meta, h, kv, w_packed),
        [pl.BlockSpec(memory_space=pltpu.SMEM), whole(h), whole(kv), pl.BlockSpec((1, n_data, q_rows, feat), lambda g: (g, 0, last, 0))],
        rows, width, n_groups, 2 * rows * d_model * width * n_groups,
        [pltpu.VMEM((rows, width), jnp.bfloat16)],
    )


def gate_heads(h, attended, w_gu, n_heads, head_dim, ff_head):
    n_groups, d_model, cols = w_gu.shape
    rows = h.shape[0]
    return group_call(
        functools.partial(gate_kernel, n_heads, head_dim, ff_head),
        (h, attended, w_gu),
        [whole(h), pl.BlockSpec((1, rows, n_heads * head_dim), lambda g: (g, 0, 0)), pl.BlockSpec((1, d_model, cols), lambda g: (g, 0, 0))],
        rows, n_heads * (head_dim + ff_head), n_groups, 2 * rows * d_model * cols * n_groups,
    )


def pack_queries(w_q):
    feat, width = w_q.shape
    return jnp.concatenate([w_q[i:i + width] for i in range(0, feat, width)], axis=1)


def project_out(x, joined, w_out, at):
    n_groups, n_data, _, width = w_out.shape
    out_loc = joined.shape[2]
    rows, d_model = x.shape
    feat = d_model // n_data
    per = n_data if n_data * width <= 2 * feat else 2
    return pl.pallas_call(
        functools.partial(out_kernel, at),
        grid=(n_data // per, n_groups),
        in_specs=[
            pl.BlockSpec((rows, per * feat), lambda c, g: (0, c)),
            pl.BlockSpec((1, rows, out_loc), lambda c, g: (g, 0, 0)),
            pl.BlockSpec((1, per, out_loc, width), lambda c, g: (g, c, 0, 0)),
        ],
        out_specs=pl.BlockSpec((rows, per * feat), lambda c, g: (0, c)),
        out_shape=jax.ShapeDtypeStruct((rows, d_model), jnp.bfloat16),
        scratch_shapes=[pltpu.VMEM((rows, per * width), jnp.float32)],
        compiler_params=pltpu.CompilerParams(vmem_limit_bytes=VMEM_LIMIT, dimension_semantics=("arbitrary", "arbitrary")),
        cost_estimate=pl.CostEstimate(flops=2 * rows * n_data * width * out_loc * n_groups, bytes_accessed=2 * w_out.size, transcendentals=0),
        name="project_out",
    )(x, joined, w_out)


def stack_by_shift(arr, axis, size, stride):
    n = size // stride

    def shift(value, r):
        return lax.ppermute(value, axis, [(i, (i + r * stride) % size) for i in range(size)])

    if n != 4:
        return jnp.stack([arr] + [shift(arr, r) for r in range(1, n)])
    back, ahead = shift(arr, 1), shift(arr, -1)
    half = arr.shape[0] // 2
    across = jnp.concatenate([shift(back[:half], 1), shift(ahead[half:], -1)])
    return jnp.stack([arr, back, across, ahead])


def absolute_order(rel, mine, n):
    return jnp.concatenate([lax.dynamic_slice_in_dim(rel, lax.rem(mine - i + n, n), 1, 0) for i in range(n)])


def swap_pair(value, n_model):
    other = lax.ppermute(value, "model", [(i, i ^ 1) for i in range(n_model)])
    first = lax.rem(lax.axis_index("model"), 2) == 0
    return jnp.where(first, value, other), jnp.where(first, other, value)


def gather_model(arr, n_model):
    mine = stack_by_shift(arr, "model", n_model, 2)
    both = jnp.stack(swap_pair(mine, n_model), axis=1)
    both = absolute_order(both, lax.axis_index("model") // 2, n_model // 2)
    return both.reshape((n_model,) + arr.shape)


def gather_kv_weights(w_kv, n_data, n_model):
    n_layers, feat, cols = w_kv.shape
    first = lax.rem(lax.axis_index("model"), 2) == 0
    half = jnp.where(first, w_kv[..., :cols // 2], w_kv[..., cols // 2:])
    half = absolute_order(stack_by_shift(half, "data", n_data, 1), lax.axis_index("data"), n_data)
    whole = jnp.concatenate(swap_pair(half, n_model), axis=-1)
    return whole.transpose(1, 0, 2, 3).reshape(n_layers, n_data * feat, cols)


def solution(mesh):
    n_model = mesh.shape["model"]
    n_data = mesh.shape["data"]
    act_spec = P(None, ("part", "data"), "model", None)
    ring = ("model", "data")

    def gather(arr):
        return lax.all_gather(arr, ring, axis=0, tiled=True)

    def layers_fn(x_blk, len_blk, gain_blk, w_in_blk, w_kv_blk, w_out_blk):
        n_layers, feat, in_loc = w_in_blk.shape
        head_dim = w_kv_blk.shape[2] // 2
        out_loc = w_out_blk.shape[1]
        heads_loc = (out_loc - (in_loc - out_loc)) // head_dim
        ff_head = out_loc // heads_loc - head_dim
        n_micro, n_seqs, t_loc, d_model = x_blk.shape
        n_batch = n_micro * n_seqs
        rows = n_batch * t_loc
        q_offset = lax.axis_index("model") * t_loc
        meta = jnp.concatenate([len_blk.reshape(n_batch), q_offset[None]]).astype(jnp.int32)

        unit_in = in_loc // heads_loc
        weights = []
        for layer in range(n_layers):
            heads = [w_in_blk[layer, :, i * unit_in:(i + 1) * unit_in] for i in range(heads_loc)]
            piece = w_in_blk[layer] if layer == 0 else jnp.concatenate([w[:, head_dim:] for w in heads], axis=1)
            w_in = gather(piece).reshape(n_model, d_model, piece.shape[1])
            w_outs = []
            last = layer == n_layers - 1
            cuts = (0, feat * 3 // 4, feat) if last else (0, feat)
            for lo, hi in zip(cuts, cuts[1:]):
                piece = w_out_blk[layer, :, lo:hi]
                if not last:
                    after = [w_in_blk[layer + 1, :, j * unit_in:j * unit_in + head_dim] for j in range(heads_loc)]
                    piece = jnp.concatenate([piece, pack_queries(jnp.concatenate(after, axis=1))])
                w_out = gather(piece)
                w_outs.append((lo, w_out.reshape((n_model, n_data) + piece.shape)))
            weights.append((w_in, w_outs))

        gain = lax.all_gather(gain_blk, "data", axis=1, tiled=True)
        w_kv = gather_kv_weights(w_kv_blk, n_data, n_model)

        hidden = x_blk.reshape(rows, d_model)
        for layer, (w_in, w_outs) in enumerate(weights):
            h = layer_norm(hidden, gain[layer])
            kv = jnp.dot(h, w_kv[layer], preferred_element_type=jnp.float32).astype(jnp.bfloat16)
            kv = gather_model(kv.reshape(n_batch, t_loc, 2 * head_dim), n_model)
            if layer == 0:
                joined = project_heads(meta, h, kv, w_in, heads_loc, head_dim, ff_head)
            else:
                attended = attend_heads(meta, h, kv, weights[layer - 1][1][-1][1], heads_loc, head_dim)
                joined = gate_heads(h, attended, w_in, heads_loc, head_dim, ff_head)
            for at, w_out in w_outs:
                out = project_out if at == 0 else project_tail
                hidden = out(hidden, joined, w_out, at)
        return hidden.reshape(x_blk.shape)

    return jax.shard_map(
        layers_fn,
        mesh=mesh,
        in_specs=(act_spec, P(None, ("part", "data")), P(None, "data"), P(None, "data", "model"), P(None, "data", None), P(None, "model", "data")),
        out_specs=act_spec,
        check_vma=False,
    )
```
